32 devices in a mesh: lat: 4 (over y, x), lon: 8 (over z, core).
Axes of the slice: x: 2, y: 2, z: 4, core: 2. Of those that a mesh axis runs over, the one named last changes fastest.
Arguments:
- atmos_features: bfloat16 [128, 256, 768], P('lat', 'lon'), may hold values from -6 to 6
- ocean_features: bfloat16 [256, 512, 192], P('lat', 'lon'), may hold values from -6 to 6
- wet_cell_mask: int32 [256, 512], P('lat', 'lon'), may hold values from 0 to 1, as said below
- overlay_cell_index: int32 [4, 256, 512], P(None, 'lat', 'lon'), may hold values from 0 to 8191, as said below
- remap_weight: float32 [4, 256, 512], P(None, 'lat', 'lon'), may hold values from 0.1 to 1
- query_key_value_weight: bfloat16 [768, 2304], replicated, may hold values from -5 to 5
- attention_out_weight: bfloat16 [768, 768], replicated, may hold values from -0.21875 to 0.21875
- feedforward_up_weight: bfloat16 [768, 3072], replicated, may hold values from -0.21875 to 0.21875
- feedforward_down_weight: bfloat16 [3072, 768], replicated, may hold values from -0.109375 to 0.109375
- attention_gain: float32 [768], replicated, may hold values from 0.25 to 1.75
- feedforward_gain: float32 [768], replicated, may hold values from 0.25 to 1.75
- flux_head_weight: bfloat16 [768, 8], replicated, may hold values from -0.21875 to 0.21875
- surface_temp_embedding: float32 [768], replicated, may hold values from -5 to 5
- forcing_lift_weight: float32 [8, 192], replicated, may hold values from -2 to 2
- depthwise_kernels: float32 [2, 49, 192], replicated, may hold values from -0.875 to 0.875
- ocean_norm_gains: float32 [2, 192], replicated, may hold values from 0.25 to 1.75
- ocean_up_weights: bfloat16 [2, 192, 768], replicated, may hold values from -0.4375 to 0.4375
- ocean_down_weights: bfloat16 [2, 768, 192], replicated, may hold values from -0.21875 to 0.21875
- surface_temp_head: float32 [192], replicated, may hold values from -0.4375 to 0.4375
Outputs:
- atmos_updated: bfloat16 [128, 256, 768], P('lat', 'lon')
- ocean_out: bfloat16 [256, 512, 192], P('lat', 'lon')
The draws below stay inside these ranges and needn't reach their ends.
Inputs may be any that keep to these rules, and one draw needn't show every extreme that they name: `wet_cell_mask`: the ocean tile of rows [i * 64, i * 64 + 64) and columns [j * 64, j * 64 + 64) and the tile 256 / 2 rows north or south of it in the same columns together hold at most 4096 wet cells; some pair holds exactly that many. `overlay_cell_index`: each entry names an atmosphere cell of the latitude band of the ocean row: ocean row r belongs to the band of atmosphere rows [(r // 64) * 32, (r // 64) * 32 + 32), and the entry is (row within the band) * 256 + column.
All inputs are finite; a program needn't handle non-finite values.
Results may differ from the reference program's by a relative error of at most 0.013.
Values may be sent and summed in bfloat16 or wider, within the bound.
No kernel may reach another device: no remote copies, remote signals or barrier semaphores. Data moves between devices by JAX's collectives and lax.ppermute only.
A program may use at most 128 MiB of HBM per device.

```python
import math
import jax
import jax.numpy as jnp
from jax import lax

MODEL_WIDTH = 768
HEADS = 12
HD = 64
FFN = 3072
NF = 8
OCEAN_CHANNELS = 192
OFF = 768
NOV = 4
WR = 8
WC = 16
BLOCKS = 2
AR = 32
OR = 64
OCOL = 64
ATMOS_ROWS = 128
ATMOS_COLUMNS = 256
OLAT = 256
OLON = 512


def draw_query_key_value_weight(key, part):
    base = jnp.clip(jax.random.normal(key, (MODEL_WIDTH, 3 * MODEL_WIDTH), jnp.float32), -5.5, 5.5) * MODEL_WIDTH ** (-0.5)
    return jnp.clip(base, -5.0, 5.0).astype(jnp.bfloat16)


def draw_wet_cell_mask(key, part):
    tiles_lat = OLAT // OR
    tiles_lon = OLON // OCOL
    half_lat = tiles_lat // 2
    cells = OR * OCOL
    key_low, key_slack, key_flip, key_rank = jax.random.split(key, 4)
    lower = jax.random.randint(key_low, (half_lat, tiles_lon), cells // 8, cells - cells // 8 + 1)
    slack = jax.random.randint(key_slack, (half_lat, tiles_lon), 0, cells // 8 + 1)
    first_tile = (jnp.arange(half_lat)[:, None] == 0) & (jnp.arange(tiles_lon)[None, :] == 0)
    slack = jnp.where(first_tile, 0, slack)
    upper = cells - lower - slack
    flipped = jax.random.randint(key_flip, (half_lat, tiles_lon), 0, 2)
    southern = jnp.where(flipped == 1, lower, upper)
    northern = jnp.where(flipped == 1, upper, lower)
    counts = jnp.concatenate([southern, northern], axis=0).reshape(-1, 1)
    tile_keys = jax.random.split(key_rank, tiles_lat * tiles_lon)
    ranks = jax.vmap(lambda single: jax.random.permutation(single, cells))(tile_keys)
    wet = (ranks < counts).astype(jnp.int32)
    wet = wet.reshape(tiles_lat, tiles_lon, OR, OCOL).transpose(0, 2, 1, 3)
    return wet.reshape(OLAT, OLON)


def draw_overlay_cell_index(key, part):
    atm_cols = OLON // 2
    keys_all = jax.random.split(key, 5)
    shape = (NOV, OLAT, OLON)
    row_shift = jax.random.randint(keys_all[0], shape, -1, 2)
    col_shift = jax.random.randint(keys_all[1], shape, -1, 2)
    ocean_rows = jnp.arange(OLAT, dtype=jnp.int32)[None, :, None]
    ocean_cols = jnp.arange(OLON, dtype=jnp.int32)[None, None, :]
    near_row = jnp.clip(ocean_rows % OR // 2 + row_shift, 0, AR - 1)
    near_col = (ocean_cols // 2 + col_shift) % atm_cols
    distant = jax.random.randint(keys_all[2], shape, 0, 8) == 0
    far_row = jax.random.randint(keys_all[3], shape, 0, AR)
    far_col = jax.random.randint(keys_all[4], shape, 0, atm_cols)
    row_pick = jnp.where(distant, far_row, near_row)
    col_pick = jnp.where(distant, far_col, near_col)
    return (row_pick * atm_cols + col_pick).astype(jnp.int32)


def shard_levels(stream_key, shape, shards, low, top_value):
    level = 1.0
    for position, shards_of in shards:
        draws = jax.random.uniform(jax.random.fold_in(jax.random.fold_in(stream_key, 6), position), (shards_of,), jnp.float32, low / len(shards), top_value / len(shards))
        level = level * jnp.repeat(jnp.exp(draws), shape[position] // shards_of).reshape((-1,) + (1,) * (len(shape) - 1 - position))
    return level


def centred(stream_key, shape, scale, bound, shards=(), held_as=jnp.bfloat16):
    loudness = shard_levels(stream_key, shape, shards, -0.22, 0.18) if shards else 1.0
    values = jax.random.normal(stream_key, shape, jnp.float32) * scale * loudness
    return jnp.minimum(jnp.maximum(values, -bound), bound).astype(held_as)


def setup_inputs(seed: int = 0) -> dict:
    key_list = jax.random.split(jax.random.key(seed), 20)
    return {
        "atmos_features": centred(key_list[0], (ATMOS_ROWS, ATMOS_COLUMNS, MODEL_WIDTH), 1.0, 6.0, ((0, 4), (1, 8))),
        "ocean_features": centred(key_list[1], (OLAT, OLON, OCEAN_CHANNELS), 1.0, 6.0, ((0, 4), (1, 8))),
        "wet_cell_mask": draw_wet_cell_mask(jax.random.fold_in(key_list[19], 71), 0),
        "overlay_cell_index": draw_overlay_cell_index(jax.random.fold_in(key_list[19], 71), 0),
        "remap_weight": jnp.clip(jnp.exp(math.log(1.0) - 2.3025851 * jax.random.uniform(key_list[4], (NOV, OLAT, OLON), jnp.float32) ** shard_levels(key_list[4], (NOV, OLAT, OLON), ((1, 4), (2, 8)), -0.2, 0.2)), 0.1, 1.0),
        "query_key_value_weight": draw_query_key_value_weight(jax.random.fold_in(key_list[19], 71), 0),
        "attention_out_weight": centred(key_list[6], (MODEL_WIDTH, MODEL_WIDTH), MODEL_WIDTH ** -0.5, 0.21875),
        "feedforward_up_weight": centred(key_list[7], (MODEL_WIDTH, FFN), MODEL_WIDTH ** -0.5, 0.21875),
        "feedforward_down_weight": centred(key_list[8], (FFN, MODEL_WIDTH), FFN ** -0.5, 0.109375),
        "attention_gain": jnp.clip(1.0 + 0.15 * jax.random.normal(key_list[9], (MODEL_WIDTH,), jnp.float32), 0.25, 1.75),
        "feedforward_gain": jnp.clip(1.0 + 0.15 * jax.random.normal(key_list[10], (MODEL_WIDTH,), jnp.float32), 0.25, 1.75),
        "flux_head_weight": centred(key_list[11], (MODEL_WIDTH, NF), MODEL_WIDTH ** -0.5, 0.21875),
        "surface_temp_embedding": centred(key_list[12], (MODEL_WIDTH,), 1.0, 5.0, (), jnp.float32),
        "forcing_lift_weight": centred(key_list[13], (NF, OCEAN_CHANNELS), NF ** -0.5, 2.0, (), jnp.float32),
        "depthwise_kernels": centred(key_list[14], (BLOCKS, 49, OCEAN_CHANNELS), 49 ** -0.5, 0.875, (), jnp.float32),
        "ocean_norm_gains": jnp.clip(1.0 + 0.15 * jax.random.normal(key_list[15], (BLOCKS, OCEAN_CHANNELS), jnp.float32), 0.25, 1.75),
        "ocean_up_weights": centred(key_list[16], (BLOCKS, OCEAN_CHANNELS, OFF), OCEAN_CHANNELS ** -0.5, 0.4375),
        "ocean_down_weights": centred(key_list[17], (BLOCKS, OFF, OCEAN_CHANNELS), OFF ** -0.5, 0.21875),
        "surface_temp_head": centred(key_list[18], (OCEAN_CHANNELS,), OCEAN_CHANNELS ** -0.5, 0.4375, (), jnp.float32),
    }


EPS = 1e-06

def rms_scale(values, gain):
    return values * lax.rsqrt(lax.optimization_barrier(jnp.mean(values * values, axis=-1, keepdims=True)) + EPS) * gain

def layer_scale(values, gain):
    center = values - lax.optimization_barrier(jnp.mean(values, axis=-1, keepdims=True))
    return center * lax.rsqrt(lax.optimization_barrier(jnp.mean(center * center, axis=-1, keepdims=True)) + EPS) * gain

def to_windows(tensor):
    row_total, column_total = (tensor.shape[0], tensor.shape[1])
    shaped = tensor.reshape(row_total // WR, WR, column_total // WC, WC, HEADS, HD)
    return shaped.transpose(0, 2, 4, 1, 3, 5).reshape(-1, HEADS, WR * WC, HD)

def from_windows(tensor, row_total, column_total):
    shaped = tensor.reshape(row_total // WR, column_total // WC, HEADS, WR, WC, HD)
    return shaped.transpose(0, 3, 1, 4, 2, 5).reshape(row_total, column_total, HEADS * HD)

def depthwise(padded, taps, row_total, column_total):
    total = jnp.zeros((row_total, column_total, padded.shape[2]), jnp.float32)
    for north in range(7):
        for east in range(7):
            window = padded[north:north + row_total, east:east + column_total].astype(jnp.float32)
            total = total + window * taps[north * 7 + east]
    return total

def atm_band(band, query_key_value_weight, attention_out_weight, feedforward_up_weight, feedforward_down_weight, attention_gain, feedforward_gain, flux_head_weight):
    model_state = band.astype(jnp.float32)
    normed = rms_scale(model_state, attention_gain).astype(jnp.bfloat16)
    projected = jnp.dot(normed, query_key_value_weight, preferred_element_type=jnp.float32).astype(jnp.bfloat16)
    rolled = jnp.roll(projected, WC // 2, axis=1)
    query = to_windows(rolled[..., :MODEL_WIDTH]).astype(jnp.float32)
    keys_win = to_windows(rolled[..., MODEL_WIDTH:2 * MODEL_WIDTH]).astype(jnp.float32)
    value_win = to_windows(rolled[..., 2 * MODEL_WIDTH:]).astype(jnp.float32)
    scores = jnp.einsum('whqd,whkd->whqk', query, keys_win) * HD ** (-0.5)
    probs = jax.nn.softmax(scores, axis=-1).astype(jnp.bfloat16)
    mixed = jnp.einsum('whqk,whkd->whqd', probs.astype(jnp.float32), value_win).astype(jnp.bfloat16)
    attended = jnp.roll(from_windows(mixed, WR, ATMOS_COLUMNS), -(WC // 2), axis=1)
    first = model_state + jnp.dot(attended, attention_out_weight, preferred_element_type=jnp.float32)
    normed_mlp = rms_scale(first, feedforward_gain).astype(jnp.bfloat16)
    active = jax.nn.gelu(jnp.dot(normed_mlp, feedforward_up_weight, preferred_element_type=jnp.float32)).astype(jnp.bfloat16)
    second_half = first + jnp.dot(active, feedforward_down_weight, preferred_element_type=jnp.float32)
    fluxes = jnp.dot(second_half.astype(jnp.bfloat16), flux_head_weight, preferred_element_type=jnp.float32).astype(jnp.bfloat16)
    return (second_half, fluxes)

def reference(atmos_features, ocean_features, wet_cell_mask, overlay_cell_index, remap_weight, query_key_value_weight, attention_out_weight, feedforward_up_weight, feedforward_down_weight, attention_gain, feedforward_gain, flux_head_weight, surface_temp_embedding, forcing_lift_weight, depthwise_kernels, ocean_norm_gains, ocean_up_weights, ocean_down_weights, surface_temp_head):
    bands = atmos_features.reshape(ATMOS_ROWS // WR, WR, ATMOS_COLUMNS, MODEL_WIDTH)
    second_half, fluxes = lax.map(lambda band: atm_band(band, query_key_value_weight, attention_out_weight, feedforward_up_weight, feedforward_down_weight, attention_gain, feedforward_gain, flux_head_weight), bands)
    second_half = second_half.reshape(ATMOS_ROWS, ATMOS_COLUMNS, MODEL_WIDTH)
    flux_flat = fluxes.reshape(ATMOS_ROWS * ATMOS_COLUMNS, NF)
    band_start = jnp.arange(OLAT, dtype=jnp.int32) // OR * (AR * ATMOS_COLUMNS)
    global_index = overlay_cell_index + band_start[None, :, None]
    picked = flux_flat[global_index].astype(jnp.float32)
    forcing = lax.optimization_barrier(jnp.sum(remap_weight[..., None] * picked, axis=0))
    wet = wet_cell_mask.astype(jnp.float32)[..., None]
    lifted = jnp.dot(forcing, forcing_lift_weight, precision=lax.Precision.HIGHEST, preferred_element_type=jnp.float32)
    model_state = wet * (ocean_features.astype(jnp.float32) + lifted)
    for block_id in range(BLOCKS):
        rounded = model_state.astype(jnp.bfloat16)
        wrapped = jnp.concatenate([rounded[:, -3:], rounded, rounded[:, :3]], axis=1)
        north_rows = wrapped[OLAT - 3:][::-1, ::-1]
        south_rows = jnp.zeros((3, OLON + 6, OCEAN_CHANNELS), jnp.bfloat16)
        padded = jnp.concatenate([south_rows, wrapped, north_rows], axis=0)
        taps = depthwise_kernels[block_id]
        gain = ocean_norm_gains[block_id]
        up_weight = ocean_up_weights[block_id]
        down_weight = ocean_down_weights[block_id]

        def band_step(band_id):
            rows_here = lax.dynamic_slice_in_dim(padded, band_id * OR, OR + 6, 0)
            convolved = depthwise(rows_here, taps, OR, OLON)
            normed = layer_scale(convolved, gain).astype(jnp.bfloat16)
            active = jax.nn.gelu(jnp.dot(normed, up_weight, preferred_element_type=jnp.float32)).astype(jnp.bfloat16)
            return jnp.dot(active, down_weight, preferred_element_type=jnp.float32)
        increment = lax.map(band_step, jnp.arange(OLAT // OR, dtype=jnp.int32)).reshape(OLAT, OLON, OCEAN_CHANNELS)
        model_state = model_state + wet * increment
    ocean_out = model_state.astype(jnp.bfloat16)
    sea_surface_temp = jnp.dot(model_state, surface_temp_head, precision=lax.Precision.HIGHEST, preferred_element_type=jnp.float32)
    numerator = sea_surface_temp.reshape(ATMOS_ROWS, 2, ATMOS_COLUMNS, 2).sum(axis=(1, 3))
    wet_cell_count = wet_cell_mask.reshape(ATMOS_ROWS, 2, ATMOS_COLUMNS, 2).sum(axis=(1, 3)).astype(jnp.float32)
    surface_temp_atmos = numerator / jnp.maximum(wet_cell_count, 1.0)
    atmos_updated = (second_half + surface_temp_atmos[..., None] * surface_temp_embedding).astype(jnp.bfloat16)
    return (atmos_updated, ocean_out)
```

```python
import functools

import jax
import jax.numpy as jnp
from jax import lax
from jax.experimental import pallas as pl
from jax.experimental.pallas import tpu as pltpu
from jax.sharding import PartitionSpec as P

HEADS = 12
HD = 64
WR = 8
WC = 16
EPS = 1e-06
LANES = 128
SUB = 8
HALO = 8
REACH = 3
F32 = jnp.float32
BF16 = jnp.bfloat16

VMEM = pl.BlockSpec(memory_space=pltpu.VMEM)
SMEM = pl.BlockSpec(memory_space=pltpu.SMEM)
HBM = pl.BlockSpec(memory_space=pl.ANY)


def gelu(x):
    inner = x * (0.7978845608028654 + 0.035677408136300125 * (x * x))
    half = 0.5 * x
    return half + half * jnp.tanh(inner)


def ring(count, step):
    return [(i, (i + step) % count) for i in range(count)]


def atmosphere_kernel(
    is_edge, x_ref, halo_ref, gains_ref, wqkv_hbm, wout_hbm, wup_hbm, wdown_hbm, wflux_ref,
    second_ref, flux_ref,
    x_s, normed_s, qkv_s, att_s, first_s, act_s, wqkv, wout, wup, wdown, sems,
):
    half = WC // 2
    copies = [
        pltpu.make_async_copy(wqkv_hbm, wqkv, sems.at[0]),
        pltpu.make_async_copy(wout_hbm, wout, sems.at[1]),
        pltpu.make_async_copy(wup_hbm, wup, sems.at[2]),
        pltpu.make_async_copy(wdown_hbm, wdown, sems.at[3]),
    ]
    for copy in copies:
        copy.start()
    rows = x_ref.shape[0]
    cols = x_ref.shape[1]
    width = x_ref.shape[2]
    cells = WR * WC
    blocks = rows // WR
    for m in range(blocks):
        own = x_ref[m * WR : (m + 1) * WR].astype(F32)
        if is_edge:
            halo = halo_ref[m * WR : (m + 1) * WR].astype(F32)
            window = jnp.concatenate([own[:, cols - half :], halo], axis=1)
        else:
            window = own[:, half : half + WC]
        flat = window.reshape(cells, width)
        x_s[m * cells : (m + 1) * cells] = flat
        scale = lax.rsqrt(jnp.mean(flat * flat, axis=-1, keepdims=True) + EPS)
        normed_s[m * cells : (m + 1) * cells] = (flat * scale * gains_ref[0:1]).astype(BF16)
    copies[0].wait()
    step = 256
    for n in range(0, wqkv.shape[1], step):
        qkv_s[:, n : n + step] = jnp.dot(
            normed_s[...], wqkv[:, n : n + step], preferred_element_type=F32
        ).astype(BF16)
    lane = lax.broadcasted_iota(jnp.int32, (cells, LANES), 1)
    low = lane < HD
    ones_low = jnp.where(low, 1.0, 0.0).astype(BF16)
    ones_high = jnp.where(low, 0.0, 1.0).astype(BF16)
    norm = HD ** (-0.5)
    mask_low = jnp.where(low, norm, 0.0).astype(BF16)
    mask_high = jnp.where(low, 0.0, norm).astype(BF16)
    for m in range(blocks):
        span = pl.ds(m * cells, cells)
        for pair in range(HEADS // 2):
            base = pair * LANES
            q = qkv_s[span, base : base + LANES]
            k = qkv_s[span, width + base : width + base + LANES]
            v = qkv_s[span, 2 * width + base : 2 * width + base + LANES]
            k2 = jnp.concatenate([k * mask_low, k * mask_high], axis=0)
            scores = lax.dot_general(
                q, k2, (((1,), (1,)), ((), ())), preferred_element_type=F32
            )
            probs = []
            for head in range(2):
                s = scores[:, head * cells : (head + 1) * cells]
                probs.append(jnp.exp(s - jnp.max(s, axis=-1, keepdims=True)).astype(BF16))
            both = jnp.concatenate(probs, axis=1)
            v2 = jnp.concatenate(
                [
                    jnp.concatenate([v * ones_low, ones_low], axis=1),
                    jnp.concatenate([v * ones_high, ones_high], axis=1),
                ],
                axis=0,
            )
            mixed = jnp.dot(both, v2, preferred_element_type=F32)
            att_s[span, base : base + LANES] = (
                mixed[:, :LANES] / mixed[:, LANES:]
            ).astype(BF16)
    copies[1].wait()
    for n in range(0, width, step):
        first_s[:, n : n + step] = x_s[:, n : n + step] + jnp.dot(
            att_s[...], wout[:, n : n + step], preferred_element_type=F32
        )
    for m in range(blocks):
        flat = first_s[m * cells : (m + 1) * cells]
        scale = lax.rsqrt(jnp.mean(flat * flat, axis=-1, keepdims=True) + EPS)
        normed_s[m * cells : (m + 1) * cells] = (flat * scale * gains_ref[1:2]).astype(BF16)
    copies[2].wait()
    for n in range(0, wup.shape[1], step):
        act_s[:, n : n + step] = gelu(
            jnp.dot(normed_s[...], wup[:, n : n + step], preferred_element_type=F32)
        ).astype(BF16)
    copies[3].wait()
    flux = None
    for n in range(0, width, step):
        second = first_s[:, n : n + step] + jnp.dot(
            act_s[...], wdown[:, n : n + step], preferred_element_type=F32
        )
        second_ref[:, n : n + step] = second
        part = lax.dot_general(
            wflux_ref[:, n : n + step],
            second.astype(BF16),
            (((1,), (1,)), ((), ())),
            preferred_element_type=F32,
        )
        flux = part if flux is None else flux + part
    for g in range(flux_ref.shape[0]):
        flux_ref[g] = flux[:, g * 256 : (g + 1) * 256].astype(BF16)


def atmosphere(is_edge, x, halo, gains, wqkv, wout, wup, wdown, wflux_t):
    rows, cols, width = x.shape
    total = rows * WC
    ffn = wup.shape[1]
    channels = wflux_t.shape[0]
    return pl.pallas_call(
        functools.partial(atmosphere_kernel, is_edge),
        out_shape=(
            jax.ShapeDtypeStruct((total, width), F32),
            jax.ShapeDtypeStruct((total // 256, channels, 256), BF16),
        ),
        in_specs=[VMEM, VMEM, VMEM, HBM, HBM, HBM, HBM, VMEM],
        out_specs=(VMEM, VMEM),
        scratch_shapes=[
            pltpu.VMEM((total, width), F32),
            pltpu.VMEM((total, width), BF16),
            pltpu.VMEM((total, 3 * width), BF16),
            pltpu.VMEM((total, width), BF16),
            pltpu.VMEM((total, width), F32),
            pltpu.VMEM((total, ffn), BF16),
            pltpu.VMEM(wqkv.shape, BF16),
            pltpu.VMEM(wout.shape, BF16),
            pltpu.VMEM(wup.shape, BF16),
            pltpu.VMEM(wdown.shape, BF16),
            pltpu.SemaphoreType.DMA((4,)),
        ],
        name="atm_edge" if is_edge else "atm_own",
    )(x, halo, gains, wqkv, wout, wup, wdown, wflux_t)


def regrid_kernel(band_cols, own_cols, table_ref, meta_ref, out_ref):
    groups = table_ref.shape[0]
    channels = table_ref.shape[1]
    depth = table_ref.shape[2]
    table = (
        table_ref[...].astype(F32).reshape(groups * channels, depth).astype(BF16)
    )
    entries = (meta_ref.shape[0] - 1) // 2
    total = meta_ref.shape[1]
    step = 640
    halves = own_cols // WC
    per_half = groups // (band_cols // own_cols * halves)
    bits = groups.bit_length() - 1

    def chunk(i, carry):
        span = pl.ds(pl.multiple_of(i * step, LANES), step)
        place = meta_ref[0:entries, span].astype(jnp.int32)
        row = place // band_cols
        col = place % band_cols
        col = jnp.where(col < WC // 2, col + band_cols, col) - WC // 2
        part = (col // WC) * per_half + row // (WR * 2)
        slot = (row % (WR * 2)) * WC + col % WC
        slot_f = slot.astype(F32)
        total_flux = None
        iota = lax.broadcasted_iota(jnp.int32, (depth, step), 0).astype(F32)
        for e in range(entries):
            hot = jnp.where(iota == slot_f[e : e + 1], 1.0, 0.0).astype(BF16)
            picked = jnp.dot(table, hot, preferred_element_type=F32)
            level = [picked[g * channels : (g + 1) * channels] for g in range(groups)]
            code = jnp.broadcast_to(part[e : e + 1], (channels, step))
            for bit in range(bits):
                odd = ((code >> bit) & 1) == 1
                level = [
                    jnp.where(odd, level[2 * g + 1], level[2 * g])
                    for g in range(len(level) // 2)
                ]
            term = level[0] * meta_ref[entries + e : entries + e + 1, span]
            total_flux = term if total_flux is None else total_flux + term
        wet = meta_ref[2 * entries : 2 * entries + 1, span]
        out_ref[0:channels, span] = total_flux * wet
        out_ref[channels : 2 * channels, span] = jnp.broadcast_to(wet, (channels, step))
        return carry

    lax.fori_loop(0, total // step, chunk, 0)


def regrid(table, meta, band_cols, own_cols):
    channels = table.shape[1]
    return pl.pallas_call(
        functools.partial(regrid_kernel, band_cols, own_cols),
        out_shape=jax.ShapeDtypeStruct((2 * channels, meta.shape[1]), F32),
        in_specs=[VMEM, VMEM],
        out_specs=VMEM,
        name="regrid",
    )(table, meta)


def ocean_kernel(
    flags_ref, own_ref, west_ref, east_ref, south_ref, north_ref, fold_ref,
    flux_ref, flux_south_ref, flux_north_ref, lift_ref, flip_ref,
    taps_ref, gains_ref, up_ref, down_ref, head_ref,
    out_ref, sst_ref,
    field_a, field_b, wet_s, planes_s, normed_s,
):
    rows, cols, channels = own_ref.shape
    wide = cols + 2 * HALO
    fluxes = flux_ref.shape[0] // 2
    upper = channels - LANES
    bottom = flags_ref[0]
    top = flags_ref[1]
    run = SUB * wide

    def assemble(flux, ocean, at):
        force = flux[0:fluxes]
        high = force.astype(BF16)
        lowp = (force - high.astype(F32)).astype(BF16)
        lhs = jnp.concatenate(
            [high.astype(F32), lowp.astype(F32), high.astype(F32), flux[fluxes:]], axis=0
        ).astype(BF16)
        lifted = lax.dot_general(
            lhs, lift_ref[...], (((0,), (0,)), ((), ())), preferred_element_type=F32
        )
        wet = lifted[:, 2 * LANES :]
        span = pl.ds(at, SUB)
        wet_s[span] = wet.reshape(SUB, wide, LANES)
        field_a[0, span] = (lifted[:, :LANES] + wet * ocean[:, :LANES]).reshape(
            SUB, wide, LANES
        )
        rest = jnp.concatenate(
            [ocean[:, LANES:], jnp.zeros((run, 2 * LANES - channels), F32)], axis=1
        )
        field_a[1, span] = (lifted[:, LANES : 2 * LANES] + wet * rest).reshape(
            SUB, wide, LANES
        )

    south = south_ref[...].astype(F32).reshape(run, channels)
    assemble(flux_south_ref[...] * bottom, south, 0)
    def middle(g, carry):
        own_rows = pl.ds(pl.multiple_of(g * SUB, SUB), SUB)
        ocean = jnp.concatenate(
            [
                west_ref[own_rows].astype(F32),
                own_ref[own_rows].astype(F32),
                east_ref[own_rows].astype(F32),
            ],
            axis=1,
        ).reshape(run, channels)
        lanes = pl.ds(pl.multiple_of(g * run, LANES), run)
        assemble(flux_ref[:, lanes], ocean, pl.multiple_of(HALO + g * SUB, SUB))
        return carry
    lax.fori_loop(0, rows // SUB, middle, 0)
    folded = [
        jnp.dot(flip_ref[...], fold_ref[SUB - 1 - k], preferred_element_type=F32)
        for k in range(SUB)
    ]
    folded = jnp.concatenate(folded, axis=0)
    north = north_ref[...].astype(F32).reshape(run, channels)
    north = jnp.where(top > 0.5, folded, north)
    flux_north = jnp.where(
        top > 0.5, flux_ref[:, rows * wide :], flux_north_ref[...]
    )
    assemble(flux_north, north, HALO + rows)

    lane = lax.broadcasted_iota(jnp.int32, (2 * SUB, LANES), 1)

    def block(index, src, dst, row0, row1, count, per_body, planes, col0):
        reach = planes + 2 * REACH

        def build(i, carry):
            for t in range(2):
                for p in range(reach):
                    at = pl.ds(col0 - REACH + p, SUB, stride=planes)
                    a = src[t, row0 - REACH + i, at, :]
                    b = src[t, row1 - REACH + i, at, :]
                    planes_s[t, i, p] = jnp.concatenate([a, b], axis=0).astype(BF16)
            return carry

        lax.fori_loop(0, count + 2 * REACH, build, 0)
        cells = planes * 2 * SUB

        def convolve(i, slot, at):
            variant = jnp.where(row1 + i >= HALO + rows, 1, 0)
            sums = [[None] * planes for _ in range(2)]
            for t in range(2):
                for p0 in range(0, planes, 4):
                    group = range(p0, min(p0 + 4, planes))
                    acc = {}
                    for a in range(7):
                        xs = {
                            p: planes_s[t, i + a, p].astype(F32)
                            for p in range(p0, group[-1] + 7)
                        }
                        for b in range(7):
                            w = taps_ref[index, variant, t, 7 * a + b].astype(F32)
                            for p in group:
                                term = xs[p + b] * w
                                acc[p] = acc[p] + term if p in acc else term
                    for p in group:
                        sums[t][p] = acc[p]
            for p in range(planes):
                lo, hi = sums[0][p], sums[1][p]
                mean = jnp.sum(lo + hi, axis=-1, keepdims=True) * (1.0 / channels)
                lo = lo - mean
                hi = jnp.where(lane < upper, hi - mean, 0.0)
                var = jnp.sum(lo * lo + hi * hi, axis=-1, keepdims=True) * (1.0 / channels)
                scale = lax.rsqrt(var + EPS)
                normed_s[slot, at + p * 2 * SUB : at + (p + 1) * 2 * SUB, :LANES] = (
                    lo * scale * gains_ref[index, 0:1]
                ).astype(BF16)
                normed_s[slot, at + p * 2 * SUB : at + (p + 1) * 2 * SUB, LANES:] = (
                    hi * scale * gains_ref[index, 1:2]
                ).astype(BF16)

        def mlp(i, slot):
            normed = normed_s[slot, 0 : per_body * cells]
            active = gelu(
                jnp.dot(normed, up_ref[index], preferred_element_type=F32)
            ).astype(BF16)
            delta = jnp.dot(active, down_ref[index], preferred_element_type=F32)
            for j in range(per_body):
                for p in range(planes):
                    for h, base in enumerate((row0, row1)):
                        at = pl.ds(col0 + p, SUB, stride=planes)
                        line = base + i + j
                        wet = wet_s[line, at, :]
                        first = j * cells + p * 2 * SUB + h * SUB
                        for t in range(2):
                            dst[t, line, at, :] = src[t, line, at, :] + wet * delta[
                                first : first + SUB, t * LANES : (t + 1) * LANES
                            ]

        def body(g, carry):
            i = g * per_body
            for j in range(per_body):
                convolve(i + j, 0, j * cells)
            mlp(i, 0)
            return carry

        lax.fori_loop(0, count // per_body, body, 0)

    half0 = (rows + 2 * REACH) // 2
    block(0, field_a, field_b, HALO - REACH, HALO - REACH + half0, half0, 5, 9, HALO - 4)
    block(1, field_b, field_a, HALO, HALO + rows // 2, rows // 2, 4, cols // SUB, HALO)

    def finish(i, carry):
        pooled = [None, None]
        count = None
        for a in range(2):
            line = HALO + 2 * i + a
            lo = field_a[0, line, pl.ds(HALO, cols), :]
            hi = field_a[1, line, pl.ds(HALO, cols), :]
            out_ref[2 * i + a] = jnp.concatenate([lo, hi[:, :upper]], axis=1).astype(BF16)
            for b in range(2):
                at = pl.ds(HALO + b, cols // 2, stride=2)
                for t in range(2):
                    value = field_a[t, line, at, :]
                    pooled[t] = value if pooled[t] is None else pooled[t] + value
                wet = wet_s[line, at, :]
                count = wet if count is None else count + wet
        dot = jnp.sum(
            pooled[0] * head_ref[0:1] + pooled[1] * head_ref[1:2], axis=-1, keepdims=True
        )
        sst_ref[i] = dot / jnp.maximum(count, 1.0)
        return carry

    lax.fori_loop(0, rows // 2, finish, 0)


def ocean(flags, pieces, flux, flux_south, flux_north, lift, flip, taps, gains, up, down, head):
    own = pieces[0]
    rows, cols, channels = own.shape
    tall = rows + 2 * HALO
    wide = cols + 2 * HALO
    return pl.pallas_call(
        ocean_kernel,
        out_shape=(
            jax.ShapeDtypeStruct((rows, cols, channels), BF16),
            jax.ShapeDtypeStruct((rows // 2, cols // 2, LANES), F32),
        ),
        in_specs=[SMEM] + [VMEM] * 16,
        out_specs=(VMEM, VMEM),
        scratch_shapes=[
            pltpu.VMEM((2, tall, wide, LANES), F32),
            pltpu.VMEM((2, tall, wide, LANES), F32),
            pltpu.VMEM((tall, wide, LANES), F32),
            pltpu.VMEM((2, rows // 2 + REACH + 2 * REACH, 15, 2 * SUB, LANES), BF16),
            pltpu.VMEM((2, 720, 2 * LANES), BF16),
        ],
        name="ocean",
    )(flags, *pieces, flux, flux_south, flux_north, lift, flip, taps, gains, up, down, head)


def update_kernel(own_ref, edge_ref, back_ref, sst_ref, embed_ref, out_ref):
    half = WC // 2
    width = own_ref.shape[1]
    cols = sst_ref.shape[1]
    own = own_ref[...].reshape(WR, WC, width)
    edge = edge_ref[...].reshape(WR, WC, width)
    back = back_ref[...].astype(F32)
    second = jnp.concatenate([back, own, edge[:, :half]], axis=1)
    sst = sst_ref[...][:, :, 0:1]
    out_ref[...] = (
        second + sst * embed_ref[...].reshape(1, 1, width)
    ).astype(BF16)


def update(own, edge, back, sst, embed, rows, cols):
    width = own.shape[1]
    cells = WR * WC
    half = WC // 2
    return pl.pallas_call(
        update_kernel,
        grid=(rows // WR,),
        out_shape=jax.ShapeDtypeStruct((rows, cols, width), BF16),
        in_specs=[
            pl.BlockSpec((cells, width), lambda m: (m, 0)),
            pl.BlockSpec((cells, width), lambda m: (m, 0)),
            pl.BlockSpec((WR, half, width), lambda m: (m, 0, 0)),
            pl.BlockSpec((WR, cols, LANES), lambda m: (m, 0, 0)),
            pl.BlockSpec((1, width), lambda m: (0, 0)),
        ],
        out_specs=pl.BlockSpec((WR, cols, width), lambda m: (m, 0, 0)),
        name="update",
    )(own, edge, back, sst, embed)


def body(
    atmos_features,
    ocean_features,
    wet_cell_mask,
    overlay_cell_index,
    remap_weight,
    query_key_value_weight,
    attention_out_weight,
    feedforward_up_weight,
    feedforward_down_weight,
    attention_gain,
    feedforward_gain,
    flux_head_weight,
    surface_temp_embedding,
    forcing_lift_weight,
    depthwise_kernels,
    ocean_norm_gains,
    ocean_up_weights,
    ocean_down_weights,
    surface_temp_head,
):
    arows, acols, width = atmos_features.shape
    rows, cols, channels = ocean_features.shape
    entries = overlay_cell_index.shape[0]
    half = WC // 2
    lat_index = lax.axis_index("lat")
    lat_count = lax.axis_size("lat")
    lon_count = lax.axis_size("lon")
    right, left = ring(lon_count, 1), ring(lon_count, -1)
    up_lat, down_lat = ring(lat_count, 1), ring(lat_count, -1)
    mirror = [(i, lon_count - 1 - i) for i in range(lon_count)]
    wide = cols + 2 * HALO
    run = SUB * wide
    is_top = lat_index == lat_count - 1

    x_halo = lax.ppermute(atmos_features[:, :half], "lon", left)
    west = lax.ppermute(ocean_features[:, cols - HALO :], "lon", right)
    east = lax.ppermute(ocean_features[:, :HALO], "lon", left)
    meta = jnp.concatenate(
        [
            overlay_cell_index.astype(F32),
            remap_weight,
            wet_cell_mask.astype(F32)[None],
        ],
        axis=0,
    )
    meta_west = lax.ppermute(meta[:, :, cols - HALO :], "lon", right)
    meta_east = lax.ppermute(meta[:, :, :HALO], "lon", left)

    gains = jnp.stack([attention_gain, feedforward_gain])
    wflux_t = flux_head_weight.T
    weights = (
        gains,
        query_key_value_weight,
        attention_out_weight,
        feedforward_up_weight,
        feedforward_down_weight,
        wflux_t,
    )
    second_own, flux_own = atmosphere(False, atmos_features, atmos_features[:, :half], *weights)

    south_strip = jnp.concatenate([west[:SUB], ocean_features[:SUB], east[:SUB]], axis=1)
    north_strip = jnp.concatenate(
        [west[rows - SUB :], ocean_features[rows - SUB :], east[rows - SUB :]], axis=1
    )
    north = lax.ppermute(south_strip, "lat", down_lat)
    south = lax.ppermute(north_strip, "lat", up_lat)
    fold = lax.ppermute(north_strip, "lon", mirror)
    meta_wide = jnp.concatenate([meta_west, meta, meta_east], axis=2).reshape(
        meta.shape[0], rows * wide
    )
    meta_fold = lax.ppermute(meta_wide[:, (rows - SUB) * wide :], "lon", mirror)[:, ::-1]
    meta_all = jnp.concatenate([meta_wide, meta_fold], axis=1)

    second_edge, flux_edge = atmosphere(True, atmos_features, x_halo, *weights)
    fluxes = jnp.concatenate([flux_own, flux_edge], axis=0)
    table = lax.all_to_all(
        jnp.broadcast_to(fluxes, (lon_count,) + fluxes.shape), "lon", 0, 0
    )
    table = table.reshape((-1,) + fluxes.shape[1:])
    back = lax.ppermute(
        second_edge.reshape(arows, WC, width)[:, half:].astype(BF16), "lon", right
    )

    flux = regrid(table, meta_all, acols * lon_count, acols)
    flux_north = lax.ppermute(flux[:, :run], "lat", down_lat)
    flux_south = lax.ppermute(
        flux[:, (rows - SUB) * wide : rows * wide], "lat", up_lat
    )

    flags = jnp.stack([lat_index != 0, is_top]).astype(F32)
    lift_high = forcing_lift_weight.astype(BF16)
    lift_low = (forcing_lift_weight - lift_high.astype(F32)).astype(BF16)
    nf = forcing_lift_weight.shape[0]
    wet_row = (jnp.arange(nf) == 0).astype(BF16)[:, None] * jnp.ones((1, LANES), BF16)
    pad = 2 * LANES - channels
    zeros = jnp.zeros((nf, pad), BF16)
    lift = jnp.concatenate(
        [
            jnp.concatenate([part, zeros, jnp.zeros((nf, LANES), BF16)], axis=1)
            for part in (lift_high, lift_high, lift_low)
        ]
        + [jnp.concatenate([jnp.zeros((nf, 2 * LANES), BF16), wet_row], axis=1)],
        axis=0,
    )
    flip = (jnp.arange(wide)[:, None] + jnp.arange(wide)[None] == wide - 1).astype(BF16)
    blocks = depthwise_kernels.shape[0]
    taps = jnp.pad(depthwise_kernels.astype(BF16), ((0, 0), (0, 0), (0, pad)))
    taps = taps.reshape(blocks, 49, 2, LANES).transpose(0, 2, 1, 3)
    turned = jnp.where(is_top, taps[:, :, ::-1], taps)
    normal = jnp.broadcast_to(taps[:, :, :, None], (blocks, 2, 49, SUB, LANES))
    turned = jnp.broadcast_to(turned[:, :, :, None], (blocks, 2, 49, SUB, LANES))
    taps = jnp.stack(
        [
            jnp.concatenate([normal, normal], axis=3),
            jnp.concatenate([normal, turned], axis=3),
        ],
        axis=1,
    )
    ocean_gains = jnp.pad(ocean_norm_gains, ((0, 0), (0, pad))).reshape(blocks, 2, LANES)
    up = jnp.pad(ocean_up_weights, ((0, 0), (0, pad), (0, 0)))
    down = jnp.pad(ocean_down_weights, ((0, 0), (0, 0), (0, pad)))
    head = jnp.pad(surface_temp_head, (0, pad)).reshape(2, LANES)

    ocean_out, sst = ocean(
        flags,
        (ocean_features, west, east, south, north, fold),
        flux,
        flux_south,
        flux_north,
        lift,
        flip,
        taps,
        ocean_gains,
        up,
        down,
        head,
    )
    atmos_updated = update(
        second_own, second_edge, back, sst, surface_temp_embedding[None], arows, acols
    )
    return (atmos_updated, ocean_out)


def solution(mesh):
    plane = P("lat", "lon", None)
    stack = P(None, "lat", "lon")
    in_specs = (plane, plane, P("lat", "lon"), stack, stack) + (P(),) * 14
    return jax.shard_map(
        body, mesh=mesh, in_specs=in_specs, out_specs=(plane, plane), check_vma=False
    )
```
